8 devices in a mesh: dp: 2 (over z, y), sp: 4 (over x, core).
Axes of the slice: x: 2, y: 2, z: 1, core: 2. Of those that a mesh axis runs over, the one named last changes fastest.
Arguments:
- latent: bfloat16 [32, 64, 64, 4], P('dp', 'sp'), parts along dimension 0
- time_emb: bfloat16 [32, 1280], P('dp'), parts along dimension 0
- w_in: bfloat16 [3, 3, 4, 320], replicated
- b_in: bfloat16 [320], replicated
- gn1_scale: bfloat16 [2, 320], replicated
- gn1_shift: bfloat16 [2, 320], replicated
- conv1_w: bfloat16 [2, 3, 3, 320, 320], replicated
- conv1_b: bfloat16 [2, 320], replicated
- temb_w: bfloat16 [2, 1280, 320], replicated
- temb_b: bfloat16 [2, 320], replicated
- gn2_scale: bfloat16 [2, 320], replicated
- gn2_shift: bfloat16 [2, 320], replicated
- conv2_w: bfloat16 [2, 3, 3, 320, 320], replicated
- conv2_b: bfloat16 [2, 320], replicated
- down_w: bfloat16 [3, 3, 320, 320], replicated
- down_b: bfloat16 [320], replicated
Outputs:
- output 1: bfloat16 [32, 64, 64, 320], P('dp', 'sp'), parts along dimension 0
- output 2: bfloat16 [32, 64, 64, 320], P('dp', 'sp'), parts along dimension 0
- output 3: bfloat16 [32, 64, 64, 320], P('dp', 'sp'), parts along dimension 0
- output 4: bfloat16 [32, 32, 32, 320], P('dp', 'sp'), parts along dimension 0
There are 2 independent parts. The reference program is written for one: setup_inputs(seed, part) draws one part's arguments, and reference() takes and returns one part's arrays. A program takes and returns all parts, laid end to end along the dimension named above; an argument that names none is the same for every part.
All inputs are finite; a program needn't handle non-finite values.
Results may differ from the reference program's by a relative error of at most 0.0134557.
Values are sent between devices in bfloat16 or wider.
A program may use at most 1 GiB of HBM per device.

```python
import jax
import jax.numpy as jnp
from jax import lax

BATCH = 16
HEIGHT = 64
WIDTH = 64
CHANNELS = 320
TEMB_DIM = 1280
LATENT_CH = 4
GROUPS = 32
LAYERS = 2
GN_EPS = 1e-5


def setup_inputs(seed: int = 0, part: int = 0) -> dict:
    part_keys = jax.random.split(jax.random.fold_in(jax.random.key(seed), part), 4)
    shared_keys = jax.random.split(jax.random.key(seed + 1), 14)
    row_pos = jnp.linspace(-1.0, 1.0, HEIGHT)[None, :, None, None]
    noise_part = jax.random.normal(part_keys[0], (BATCH, HEIGHT, WIDTH, LATENT_CH), jnp.float32)
    row_slope = 1.5 * jax.random.normal(part_keys[1], (BATCH, 1, 1, LATENT_CH), jnp.float32)
    row_curve = jax.random.normal(part_keys[2], (BATCH, 1, 1, LATENT_CH), jnp.float32)
    latent = noise_part + row_slope * row_pos + row_curve * (1.5 * row_pos * row_pos - 0.5)
    time_emb = jax.random.normal(part_keys[3], (BATCH, TEMB_DIM), jnp.float32)
    conv_std = 1.2 * (9 * CHANNELS) ** -0.5

    def draw_w(key_slot, arr_shape, spread, center):
        return (center + spread * jax.random.normal(shared_keys[key_slot], arr_shape, jnp.float32)).astype(jnp.bfloat16)

    return {
        "latent": latent.astype(jnp.bfloat16),
        "time_emb": time_emb.astype(jnp.bfloat16),
        "w_in": draw_w(0, (3, 3, LATENT_CH, CHANNELS), (9 * LATENT_CH) ** -0.5, 0.0),
        "b_in": draw_w(1, (CHANNELS,), 0.5, 0.0),
        "gn1_scale": draw_w(2, (LAYERS, CHANNELS), 0.3, 1.0),
        "gn1_shift": draw_w(3, (LAYERS, CHANNELS), 0.3, 0.0),
        "conv1_w": draw_w(4, (LAYERS, 3, 3, CHANNELS, CHANNELS), conv_std, 0.0),
        "conv1_b": draw_w(5, (LAYERS, CHANNELS), 0.3, 0.0),
        "temb_w": draw_w(6, (LAYERS, TEMB_DIM, CHANNELS), TEMB_DIM ** -0.5, 0.0),
        "temb_b": draw_w(7, (LAYERS, CHANNELS), 0.3, 0.0),
        "gn2_scale": draw_w(8, (LAYERS, CHANNELS), 0.3, 1.0),
        "gn2_shift": draw_w(9, (LAYERS, CHANNELS), 0.3, 0.0),
        "conv2_w": draw_w(10, (LAYERS, 3, 3, CHANNELS, CHANNELS), conv_std, 0.0),
        "conv2_b": draw_w(11, (LAYERS, CHANNELS), 0.3, 0.0),
        "down_w": draw_w(12, (3, 3, CHANNELS, CHANNELS), (9 * CHANNELS) ** -0.5, 0.0),
        "down_b": draw_w(13, (CHANNELS,), 0.3, 0.0),
    }


def conv_same(inputs, kernel, bias_c, stride):
    out_f32 = lax.conv_general_dilated(inputs[None].astype(jnp.float32), kernel.astype(jnp.float32), (stride, stride), ((1, 1), (1, 1)), dimension_numbers=("NHWC", "HWIO", "NHWC"))
    return (out_f32[0] + bias_c.astype(jnp.float32)).astype(jnp.bfloat16)


def norm_silu(values, gain_c, shift_c):
    grouped = values.reshape(values.shape[0] * values.shape[1], GROUPS, CHANNELS // GROUPS)
    grp_mean = jnp.mean(grouped, axis=(0, 2), keepdims=True)
    grp_var = jnp.mean(jnp.square(grouped - grp_mean), axis=(0, 2), keepdims=True)
    normed = ((grouped - grp_mean) * lax.rsqrt(grp_var + GN_EPS)).reshape(values.shape)
    normed = normed * gain_c.astype(jnp.float32) + shift_c.astype(jnp.float32)
    return jax.nn.silu(normed).astype(jnp.bfloat16)


def reference(latent, time_emb, w_in, b_in, gn1_scale, gn1_shift, conv1_w, conv1_b, temb_w, temb_b, gn2_scale, gn2_shift, conv2_w, conv2_b, down_w, down_b):
    layer_params = (gn1_scale, gn1_shift, conv1_w, conv1_b, temb_w, temb_b, gn2_scale, gn2_shift, conv2_w, conv2_b)

    def one_sample(sample):
        latent_s, temb_s = sample
        first_out = conv_same(latent_s, w_in, b_in, 1)
        emb_act = jax.nn.silu(temb_s.astype(jnp.float32)).astype(jnp.bfloat16)

        def layer_step(hidden, params):
            norm_g1, norm_b1, conv_w1, conv_b1, proj_w, proj_b, norm_g2, norm_b2, conv_w2, conv_b2 = params
            branch = conv_same(norm_silu(hidden.astype(jnp.float32), norm_g1, norm_b1), conv_w1, conv_b1, 1)
            emb_proj = jnp.dot(emb_act.astype(jnp.float32), proj_w.astype(jnp.float32)) + proj_b.astype(jnp.float32)
            mixed_in = branch.astype(jnp.float32) + emb_proj
            branch = conv_same(norm_silu(mixed_in, norm_g2, norm_b2), conv_w2, conv_b2, 1)
            hidden = (hidden.astype(jnp.float32) + branch.astype(jnp.float32)).astype(jnp.bfloat16)
            return hidden, hidden

        last_out, per_layer = lax.scan(layer_step, first_out, layer_params)
        return first_out, per_layer, conv_same(last_out, down_w, down_b, 2)

    firsts, layers_out, down_outs = lax.map(one_sample, (latent, time_emb))
    return firsts, layers_out[:, 0], layers_out[:, 1], down_outs
```

```python
import functools

import jax
import jax.numpy as jnp
from jax import lax
from jax.experimental import pallas as pl
from jax.experimental.pallas import tpu as pltpu
from jax.sharding import PartitionSpec as P

F32 = jnp.float32
BF16 = jnp.bfloat16
GROUPS = 32
EPS = 1e-5
CH = 320
LANES = ((0, 128), (128, 256), (256, 320))
TRANS_B = (((1,), (1,)), ((), ()))
VMEM_LIMIT = 60 * 1024 * 1024


def f32_dot(a, b):
    return jnp.dot(a, b, preferred_element_type=F32, precision=lax.Precision.HIGHEST)


def group_matrix(first, chan_major):
    shape = (CH, 128) if chan_major else (128, CH)
    chan = lax.broadcasted_iota(jnp.int32, shape, 0 if chan_major else 1)
    grp = lax.broadcasted_iota(jnp.int32, shape, 1 if chan_major else 0) - first
    size = CH // GROUPS
    hit = (chan >= grp * size) & (chan < grp * size + size) & (grp >= 0) & (grp < GROUPS)
    return hit.astype(F32)


def transpose_weights(w_ref, wt_ref):
    for dy in range(3):
        for dx in range(3):
            wt_ref[dy, :, dx * 256:(dx + 1) * 256] = w_ref[dy, dx, 0:256, :].T
        rest = [w_ref[dy, dx, 256:320, :] for dx in range(3)]
        rest.append(jnp.zeros((64, CH), BF16))
        wt_ref[dy, :, 768:1024] = jnp.concatenate(rest, axis=0).T


def column_masks(cols):
    pos = lax.broadcasted_iota(jnp.int32, (cols, 128), 0)
    return pos == 0, pos == cols - 1


def put_shifted(x_ref, row0, cols, tile, left, mid, right):
    rows = pl.ds(row0, cols)
    if tile < 2:
        for dx, part in enumerate((left, mid, right)):
            x_ref[rows, dx * 256 + tile * 128:dx * 256 + tile * 128 + 128] = part.astype(BF16)
    else:
        x_ref[rows, 768:896] = jnp.concatenate([left, mid], axis=-1).astype(BF16)
        x_ref[rows, 896:1024] = jnp.concatenate([right, jnp.zeros_like(right)], axis=-1).astype(BF16)


def norm_rows(x_ref, get_row, scale, offset, rows, top, bottom, first, last):
    cols = 64
    at_left, at_right = column_masks(cols)
    for r in rows:
        for tile, (lo, hi) in enumerate(LANES):
            y = get_row(r, lo, hi).astype(F32) * scale[:, lo:hi] + offset[:, lo:hi]
            v = y * jnp.tanh(y) + y
            if r == first:
                v = jnp.where(top, jnp.zeros_like(v), v)
            if r == last:
                v = jnp.where(bottom, jnp.zeros_like(v), v)
            left = jnp.where(at_left[:, :hi - lo], 0.0, pltpu.roll(v, 1, 0))
            right = jnp.where(at_right[:, :hi - lo], 0.0, pltpu.roll(v, cols - 1, 0))
            put_shifted(x_ref, r * cols, cols, tile, left, v, right)


def fold8(v):
    return v.reshape(v.shape[0] // 8, 8, v.shape[1]).sum(axis=0)


def stage_kernel(x_first, x_odd, x_even, halo_a, halo_b, stats_in, vecs, w_ref, *rest, emb_in, emb_out, residual, want_stats, samples, count):
    rest = list(rest)
    emb_in_ref = rest.pop(0) if emb_in else None
    emb_out_ref = rest.pop(0) if emb_out else None
    res_ref = rest.pop(0) if residual else None
    out_ref = rest.pop(0)
    stats_out = rest.pop(0) if want_stats else None
    wt_ref, xa, xb, acc, scale_ref, offset_ref, sum_ref, sq_ref = rest
    step = pl.program_id(0)
    sp = lax.axis_index("sp")
    top, bottom = sp == 0, sp == lax.axis_size("sp") - 1

    def normalize(dst, src, sample, rows):
        scale = scale_ref[pl.ds(sample, 1), :]
        offset = offset_ref[pl.ds(sample, 1), :]

        def get_row(r, lo, hi):
            if r == 0:
                return halo_a[sample, :, lo:hi]
            if r == 17:
                return halo_b[sample, :, lo:hi]
            return src[0, r - 1, :, lo:hi]

        norm_rows(dst, get_row, scale, offset, rows, top, bottom, 0, 17)

    @pl.when(step == 0)
    def _():
        transpose_weights(w_ref, wt_ref)
        total = stats_in[0]
        for d in range(1, stats_in.shape[0]):
            total = total + stats_in[d]
        total = total * (1.0 / count)
        mean = total
        var = pltpu.roll(total, 128 - GROUPS, 1) - mean * mean
        inv = lax.rsqrt(var + EPS)
        expand = group_matrix(0, False)
        lane = lax.broadcasted_iota(jnp.int32, inv.shape, 1)
        inv = jnp.where(lane < GROUPS, inv, 0.0)
        mean = jnp.where(lane < GROUPS, mean, 0.0)
        scale = f32_dot(inv, expand) * vecs[0:1, :]
        mean = f32_dot(mean, expand)
        if emb_in:
            mean = mean - emb_in_ref[...]
        offset = vecs[1:2, :] - mean * scale
        scale_ref[...] = scale * 0.5
        offset_ref[...] = offset * 0.5
        normalize(xa, x_first, 0, range(18))

    bias = vecs[2:3, :]
    for sub, (cur, nxt, src) in enumerate(((xa, xb, x_odd), (xb, xa, x_even))):
        sample = step * 2 + sub
        nxt_sample = jnp.minimum(sample + 1, samples - 1)
        for half in range(2):
            total = None
            for dy in range(3):
                part = lax.dot_general(wt_ref[dy], cur[pl.ds((8 * half + dy) * 64, 512), :], TRANS_B, preferred_element_type=F32)
                total = part if total is None else total + part
            acc[2 * sub + half] = total
        normalize(nxt, src, nxt_sample, range(18))
        tot = jnp.zeros((8, CH), F32)
        tot_sq = jnp.zeros((8, CH), F32)
        for pair in range(8):
            half, part = pair // 4, pair % 4
            t = acc[2 * sub + half, :, part * 128:(part + 1) * 128].T + bias
            u = t.astype(BF16)
            if residual:
                u = (res_ref[sub, 2 * pair:2 * pair + 2].reshape(128, CH).astype(F32) + u.astype(F32)).astype(BF16)
            out_ref[sub, 2 * pair:2 * pair + 2] = u.reshape(2, 64, CH)
            if want_stats:
                v = u.astype(F32)
                if emb_out:
                    v = v + emb_out_ref[pl.ds(sample, 1), :]
                tot = tot + fold8(v)
                tot_sq = tot_sq + fold8(v * v)
        if want_stats:
            sum_ref[pl.ds(sample, 1), :] = tot.sum(axis=0, keepdims=True)
            sq_ref[pl.ds(sample, 1), :] = tot_sq.sum(axis=0, keepdims=True)

    if want_stats:
        @pl.when(step == pl.num_programs(0) - 1)
        def _():
            stats_out[...] = f32_dot(sum_ref[...], group_matrix(0, True)) + f32_dot(sq_ref[...], group_matrix(GROUPS, True))


def once(shape):
    return pl.BlockSpec(shape, lambda g: (0,) * len(shape), pipeline_mode=pl.Buffered(1))


def conv_stage(x, halo_a, halo_b, stats_in, vecs, w, *, emb_in=None, emb_out=None, residual=None, want_stats=True):
    samples, rows, cols, chans = x.shape
    count = float(rows * stats_in.shape[0] * cols * (chans // GROUPS))
    one = (1, rows, cols, chans)
    two = (2, rows, cols, chans)
    args = [x, x, x, halo_a, halo_b, stats_in, vecs, w]
    specs = [
        once(one),
        pl.BlockSpec(one, lambda g: (2 * g + 1, 0, 0, 0)),
        pl.BlockSpec(one, lambda g: (jnp.minimum(2 * g + 2, samples - 1), 0, 0, 0)),
        once(halo_a.shape), once(halo_b.shape), once(stats_in.shape), once(vecs.shape), once(w.shape),
    ]
    for emb in (emb_in, emb_out):
        if emb is not None:
            args.append(emb)
            specs.append(once(emb.shape))
    if residual is not None:
        args.append(residual)
        specs.append(pl.BlockSpec(two, lambda g: (g, 0, 0, 0)))
    out_shape = [jax.ShapeDtypeStruct(x.shape, BF16)]
    out_specs = [pl.BlockSpec(two, lambda g: (g, 0, 0, 0))]
    if want_stats:
        out_shape.append(jax.ShapeDtypeStruct((samples, 128), F32))
        out_specs.append(pl.BlockSpec((samples, 128), lambda g: (0, 0)))
    body = functools.partial(stage_kernel, emb_in=emb_in is not None, emb_out=emb_out is not None, residual=residual is not None, want_stats=want_stats, samples=samples, count=count)
    return pl.pallas_call(
        body,
        grid=(samples // 2,),
        in_specs=specs,
        out_specs=out_specs,
        out_shape=out_shape,
        scratch_shapes=[
            pltpu.VMEM((3, CH, 1024), BF16),
            pltpu.VMEM((18 * 64, 1024), BF16),
            pltpu.VMEM((18 * 64, 1024), BF16),
            pltpu.VMEM((4, CH, 512), F32),
            pltpu.VMEM((samples, CH), F32),
            pltpu.VMEM((samples, CH), F32),
            pltpu.VMEM((samples, CH), F32),
            pltpu.VMEM((samples, CH), F32),
        ],
        compiler_params=pltpu.CompilerParams(vmem_limit_bytes=VMEM_LIMIT),
        name="conv_stage",
    )(*args)


def first_kernel(lat_ref, w_ref, vecs, out_ref, halo_a, halo_b, stats_out, patch, acc, sum_ref, sq_ref):
    step = pl.program_id(0)
    lane = lax.broadcasted_iota(jnp.int32, (4, 128), 1)
    col = lane & 63
    shifted = {}
    for r in range(20):
        row = lat_ref[0, r]
        both = jnp.concatenate([row, row], axis=-1)
        for dx in range(3):
            moved = both if dx == 1 else pltpu.roll(both, 1 if dx == 0 else 127, 1)
            if dx == 0:
                moved = jnp.where(col == 0, 0.0, moved)
            if dx == 2:
                moved = jnp.where(col == 63, 0.0, moved)
            shifted[r, dx] = moved
    for pair in range(9):
        parts = []
        for dy in range(3):
            for dx in range(3):
                parts.append(jnp.where(lane < 64, shifted[2 * pair + dy, dx], shifted[2 * pair + 1 + dy, dx]))
                parts.append(jnp.zeros((4, 128), F32))
        parts += [jnp.zeros((4, 128), F32)] * 2
        patch[:, pair * 128:(pair + 1) * 128] = jnp.concatenate(parts, axis=0).astype(BF16)
    acc[...] = jnp.dot(w_ref[...], patch[...], preferred_element_type=F32)
    bias = vecs[2:3, :]
    tot = jnp.zeros((8, CH), F32)
    tot_sq = jnp.zeros((8, CH), F32)
    for pair in range(9):
        u = (acc[:, pair * 128:(pair + 1) * 128].T + bias).astype(BF16)
        upper, lower = u[:64], u[64:]
        if pair == 0:
            halo_a[0] = upper
        else:
            out_ref[0, 2 * pair - 1] = upper
        if pair == 8:
            halo_b[0] = lower
        else:
            out_ref[0, 2 * pair] = lower
        v = u.astype(F32)
        if pair == 0:
            v = v[64:]
        if pair == 8:
            v = v[:64]
        tot = tot + fold8(v)
        tot_sq = tot_sq + fold8(v * v)
    sum_ref[pl.ds(step, 1), :] = tot.sum(axis=0, keepdims=True)
    sq_ref[pl.ds(step, 1), :] = tot_sq.sum(axis=0, keepdims=True)

    @pl.when(step == pl.num_programs(0) - 1)
    def _():
        stats_out[...] = f32_dot(sum_ref[...], group_matrix(0, True)) + f32_dot(sq_ref[...], group_matrix(GROUPS, True))


def first_conv(lat, w_in, vecs):
    samples = lat.shape[0]
    w = jnp.pad(w_in.reshape(9, 4, CH), ((0, 1), (0, 4), (0, 0))).reshape(80, CH).T
    return pl.pallas_call(
        first_kernel,
        grid=(samples,),
        in_specs=[pl.BlockSpec((1,) + lat.shape[1:], lambda s: (s, 0, 0, 0)), once(w.shape), once(vecs.shape)],
        out_specs=[
            pl.BlockSpec((1, 16, 64, CH), lambda s: (s, 0, 0, 0)),
            pl.BlockSpec((1, 64, CH), lambda s: (s, 0, 0)),
            pl.BlockSpec((1, 64, CH), lambda s: (s, 0, 0)),
            pl.BlockSpec((samples, 128), lambda s: (0, 0)),
        ],
        out_shape=[
            jax.ShapeDtypeStruct((samples, 16, 64, CH), BF16),
            jax.ShapeDtypeStruct((samples, 64, CH), BF16),
            jax.ShapeDtypeStruct((samples, 64, CH), BF16),
            jax.ShapeDtypeStruct((samples, 128), F32),
        ],
        scratch_shapes=[
            pltpu.VMEM((80, 18 * 64), BF16),
            pltpu.VMEM((CH, 18 * 64), F32),
            pltpu.VMEM((samples, CH), F32),
            pltpu.VMEM((samples, CH), F32),
        ],
        compiler_params=pltpu.CompilerParams(vmem_limit_bytes=VMEM_LIMIT),
        name="conv_in",
    )(lat, w, vecs)


def down_kernel(x_ref, halo_a, vecs, w_ref, out_ref, wt_ref, xe, xo, wide, acc):
    step = pl.program_id(0)
    top = lax.axis_index("sp") == 0
    at_left, _ = column_masks(32)

    @pl.when(step == 0)
    def _():
        transpose_weights(w_ref, wt_ref)

    bias = vecs[2:3, :]
    for sub in range(2):
        for r in range(17):
            dst, row0 = (xe, 32 * (r // 2)) if r % 2 == 0 else (xo, 32 * (r // 2))
            for tile, (lo, hi) in enumerate(LANES):
                v = halo_a[step * 2 + sub, :, lo:hi] if r == 0 else x_ref[sub, r - 1, :, lo:hi]
                v = v.astype(F32)
                if r == 0:
                    v = jnp.where(top, jnp.zeros_like(v), v)
                slot = (r * 3 + tile) % 8
                wide[slot, :, 0:hi - lo] = v
                even = wide[slot, pl.ds(0, 32, stride=2), 0:hi - lo]
                odd = wide[slot, pl.ds(1, 32, stride=2), 0:hi - lo]
                left = jnp.where(at_left[:, :hi - lo], 0.0, pltpu.roll(odd, 1, 0))
                put_shifted(dst.at[sub], row0, 32, tile, left, even, odd)
        total = None
        for dy, src in enumerate((xe.at[sub, pl.ds(0, 256)], xo.at[sub], xe.at[sub, pl.ds(32, 256)])):
            part = lax.dot_general(wt_ref[dy], src[...], TRANS_B, preferred_element_type=F32)
            total = part if total is None else total + part
        acc[sub] = total
        for part in range(2):
            u = (acc[sub, :, part * 128:(part + 1) * 128].T + bias).astype(BF16)
            out_ref[sub, 4 * part:4 * part + 4] = u.reshape(4, 32, CH)


def down_conv(x, halo_a, vecs, w):
    samples = x.shape[0]
    return pl.pallas_call(
        down_kernel,
        grid=(samples // 2,),
        in_specs=[pl.BlockSpec((2, 16, 64, CH), lambda g: (g, 0, 0, 0)), once(halo_a.shape), once(vecs.shape), once(w.shape)],
        out_specs=pl.BlockSpec((2, 8, 32, CH), lambda g: (g, 0, 0, 0)),
        out_shape=jax.ShapeDtypeStruct((samples, 8, 32, CH), BF16),
        scratch_shapes=[
            pltpu.VMEM((3, CH, 1024), BF16),
            pltpu.VMEM((2, 9 * 32, 1024), BF16),
            pltpu.VMEM((2, 8 * 32, 1024), BF16),
            pltpu.VMEM((8, 64, 128), F32),
            pltpu.VMEM((2, CH, 256), F32),
        ],
        compiler_params=pltpu.CompilerParams(vmem_limit_bytes=VMEM_LIMIT),
        name="down",
    )(x, halo_a, vecs, w)


def exchange_kernel(*refs, peers, stats, above, below):
    refs = list(refs)
    stats_ref = refs.pop(0) if stats else None
    x_ref = refs.pop(0) if above or below else None
    all_ref = refs.pop(0) if stats else None
    halo_a = refs.pop(0) if above else None
    halo_b = refs.pop(0) if below else None
    s_send, s_recv, h_send, h_recv = refs
    me = lax.axis_index("sp")
    barrier = pltpu.get_barrier_semaphore()
    for d in range(1, peers):
        pl.semaphore_signal(barrier, inc=1, device_id={"sp": lax.rem(me + d, peers)}, device_id_type=pl.DeviceIdType.MESH)
    pl.semaphore_wait(barrier, peers - 1)
    copies = []
    if stats:
        for d in range(1, peers):
            copy = pltpu.make_async_remote_copy(stats_ref, all_ref.at[me], s_send.at[d], s_recv.at[d], device_id={"sp": lax.rem(me + d, peers)}, device_id_type=pl.DeviceIdType.MESH)
            copy.start()
            copies.append(copy)
    last = x_ref.shape[1] - 1 if above or below else 0
    down_copy = up_copy = None
    if above:
        down_copy = pltpu.make_async_remote_copy(x_ref.at[:, last], halo_a, h_send.at[0], h_recv.at[0], device_id={"sp": lax.rem(me + 1, peers)}, device_id_type=pl.DeviceIdType.MESH)
        pl.when(me < peers - 1)(lambda: down_copy.start())
    if below:
        up_copy = pltpu.make_async_remote_copy(x_ref.at[:, 0], halo_b, h_send.at[1], h_recv.at[1], device_id={"sp": lax.rem(me + peers - 1, peers)}, device_id_type=pl.DeviceIdType.MESH)
        pl.when(me > 0)(lambda: up_copy.start())
    if stats:
        all_ref[me] = stats_ref[...]
    for copy in copies:
        copy.wait()
    if above:
        pl.when(me < peers - 1)(lambda: down_copy.wait_send())
        pl.when(me > 0)(lambda: down_copy.wait_recv())
    if below:
        pl.when(me > 0)(lambda: up_copy.wait_send())
        pl.when(me < peers - 1)(lambda: up_copy.wait_recv())


def exchange(peers, collective_id, stats=None, x=None, above=False, below=False):
    args, in_specs, out_shape, out_specs = [], [], [], []
    if stats is not None:
        args.append(stats)
        in_specs.append(pl.BlockSpec(memory_space=pltpu.VMEM))
        out_shape.append(jax.ShapeDtypeStruct((peers,) + stats.shape, F32))
        out_specs.append(pl.BlockSpec(memory_space=pltpu.VMEM))
    if x is not None:
        args.append(x)
        in_specs.append(pl.BlockSpec(memory_space=pl.ANY))
        for want in (above, below):
            if want:
                out_shape.append(jax.ShapeDtypeStruct((x.shape[0],) + x.shape[2:], x.dtype))
                out_specs.append(pl.BlockSpec(memory_space=pl.ANY))
    return pl.pallas_call(
        functools.partial(exchange_kernel, peers=peers, stats=stats is not None, above=above, below=below),
        in_specs=in_specs,
        out_specs=out_specs,
        out_shape=out_shape,
        scratch_shapes=[pltpu.SemaphoreType.DMA((peers,)), pltpu.SemaphoreType.DMA((peers,)), pltpu.SemaphoreType.DMA((2,)), pltpu.SemaphoreType.DMA((2,))],
        compiler_params=pltpu.CompilerParams(collective_id=collective_id, has_side_effects=True),
        name="exchange",
    )(*args)


def solution(mesh):
    peers = mesh.shape["sp"]
    to_next = [(d, d + 1) for d in range(peers - 1)]
    to_prev = [(d + 1, d) for d in range(peers - 1)]

    def vectors(*rows):
        rows = [r.astype(F32) for r in rows]
        rows += [jnp.zeros((CH,), F32)] * (8 - len(rows))
        return jnp.stack(rows)

    def band_program(latent, time_emb, w_in, b_in, gn1_scale, gn1_shift, conv1_w, conv1_b, temb_w, temb_b, gn2_scale, gn2_shift, conv2_w, conv2_b, down_w, down_b):
        emb_act = jax.nn.silu(time_emb.astype(F32)).astype(BF16)
        embs = [jnp.dot(emb_act, temb_w[i], preferred_element_type=F32) + temb_b[i].astype(F32) for i in range(2)]
        lat = latent.transpose(0, 1, 3, 2)
        above = lax.ppermute(lat[:, -2:], "sp", to_next)
        below = lax.ppermute(lat[:, :2], "sp", to_prev)
        lat = jnp.concatenate([above, lat, below], axis=1).astype(F32)
        zero = jnp.zeros((CH,), BF16)
        hidden, halo_a, halo_b, stats = first_conv(lat, w_in, vectors(zero, zero, b_in))
        outputs = [hidden]
        for i in range(2):
            vec1 = vectors(gn1_scale[i], gn1_shift[i], conv1_b[i])
            vec2 = vectors(gn2_scale[i], gn2_shift[i], conv2_b[i])
            if i == 0:
                (stats_all,) = exchange(peers, 0, stats=stats)
            else:
                stats_all, halo_a, halo_b = exchange(peers, 3 * i, stats=stats, x=hidden, above=True, below=True)
            branch, stats = conv_stage(hidden, halo_a, halo_b, stats_all, vec1, conv1_w[i], emb_out=embs[i])
            stats_all, halo_a, halo_b = exchange(peers, 3 * i + 1, stats=stats, x=branch, above=True, below=True)
            got = conv_stage(branch, halo_a, halo_b, stats_all, vec2, conv2_w[i], emb_in=embs[i], residual=hidden, want_stats=i == 0)
            hidden = got[0]
            stats = got[1] if i == 0 else None
            outputs.append(hidden)
        (halo_a,) = exchange(peers, 7, x=hidden, above=True)
        outputs.append(down_conv(hidden, halo_a, vectors(zero, zero, down_b), down_w))
        return tuple(outputs)

    band = P("dp", "sp", None, None)
    return jax.shard_map(band_program, mesh=mesh, in_specs=(band, P("dp", None)) + (P(),) * 14, out_specs=(band,) * 4, check_vma=False)
```

```python
import functools

import jax
import jax.numpy as jnp
from jax import lax
from jax.experimental import pallas as pl
from jax.experimental.pallas import tpu as pltpu
from jax.sharding import PartitionSpec as P

F32 = jnp.float32
BF16 = jnp.bfloat16
GROUPS = 32
EPS = 1e-5
LANE = 128
COLS = 64
FULL = 256
DEEP = 1024
ROWS = 16
CH = 320
WIDE = ((0, FULL), (FULL, 320))
TRANS_B = (((1,), (1,)), ((), ()))
VMEM_LIMIT = 60 * DEEP * DEEP


def f32_dot(a, b):
    return jnp.dot(a, b, preferred_element_type=F32, precision=lax.Precision.HIGHEST)


def group_matrix(first, chan_major):
    shape = (CH, LANE) if chan_major else (LANE, CH)
    chan = lax.broadcasted_iota(jnp.int32, shape, 0 if chan_major else 1)
    grp = lax.broadcasted_iota(jnp.int32, shape, 1 if chan_major else 0) - first
    size = CH // GROUPS
    hit = (chan >= grp * size) & (chan < grp * size + size) & (grp >= 0) & (grp < GROUPS)
    return hit.astype(F32)


def transpose_weights(w_ref, wt_ref):
    for dy in range(3):
        for dx in range(3):
            wt_ref[dy, :, dx * FULL:(dx + 1) * FULL] = w_ref[0, dy, dx, 0:FULL, :].T
        rest = [w_ref[0, dy, dx, FULL:320, :] for dx in range(3)]
        rest.append(jnp.zeros((COLS, CH), BF16))
        wt_ref[dy, :, 768:DEEP] = jnp.concatenate(rest, axis=0).T


def put_shifted(x_ref, row0, cols, tile, left, mid, right):
    rows = pl.ds(row0, cols)
    if tile == 0:
        for dx, part in enumerate((left, mid, right)):
            x_ref[rows, dx * FULL:dx * FULL + FULL] = part.astype(BF16)
    else:
        x_ref[rows, 768:DEEP] = jnp.concatenate([left, mid, right, jnp.zeros_like(right)], axis=-1).astype(BF16)


def norm_rows(x_ref, get_row, scale, offset, rows, top, bottom, first, last):
    cols = COLS
    for r in rows:
        for tile, (lo, hi) in enumerate(WIDE):
            y = get_row(r, lo, hi).astype(F32) * scale[:, lo:hi] + offset[:, lo:hi]
            v = y * jnp.tanh(y) + y
            if r == first:
                v = jnp.where(top, jnp.zeros_like(v), v)
            if r == last:
                v = jnp.where(bottom, jnp.zeros_like(v), v)
            padded = jnp.concatenate([v, jnp.zeros((8, hi - lo), F32)], axis=0)
            left = pltpu.roll(padded, 1, 0)[:cols]
            right = pltpu.roll(padded, cols + 7, 0)[:cols]
            put_shifted(x_ref, r * cols, cols, tile, left, v, right)


def fold8(v):
    return v.reshape(v.shape[0] // 8, 8, v.shape[1]).sum(axis=0)


def row_vector(ref, layer):
    return ref[...].astype(F32)[layer:layer + 1, :]


def remote(src, dst, send, recv, peer):
    return pltpu.make_async_remote_copy(src, dst, send, recv, device_id={"sp": peer}, device_id_type=pl.DeviceIdType.MESH)


def greet(me, peers):
    barrier = pltpu.get_barrier_semaphore()
    for d in range(1, peers):
        pl.semaphore_signal(barrier, inc=1, device_id={"sp": lax.rem(me + d, peers)}, device_id_type=pl.DeviceIdType.MESH)
    pl.semaphore_wait(barrier, peers - 1)


def to_all(src, slots, send, recv, me, peers):
    return [remote(src, slots.at[me], send.at[d], recv.at[d], lax.rem(me + d, peers)) for d in range(1, peers)]


class RowSend:
    def __init__(self, src, dst, send, recv, me, peers, step):
        self.copy = remote(src, dst, send, recv, lax.rem(me + peers + step, peers))
        self.sends = me < peers - 1 if step == 1 else me > 0
        self.receives = me > 0 if step == 1 else me < peers - 1

    def start(self):
        pl.when(self.sends)(lambda: self.copy.start())

    def wait_send(self):
        pl.when(self.sends)(lambda: self.copy.wait_send())

    def wait_recv(self):
        pl.when(self.receives)(lambda: self.copy.wait_recv())


HALO_GROUPS = ((0, 1), (1, 2), (3, 4), (7, 9))
HALO_STEPS = (None, 0, 1, 3)


def stage_kernel(*refs, layer, talk, halo_in, emb_in, emb_out, residual, want_stats, samples, count, peers):
    refs = list(refs)

    def take(wanted=True):
        return refs.pop(0) if wanted else None

    x_first, x_odd, x_even = take(), take(), take()
    halo_a, halo_b = take(not halo_in), take(not halo_in)
    x_any = take(halo_in)
    stats_in, gain_ref, shift_ref, bias_ref, w_ref = take(), take(), take(), take(), take()
    emb_in_ref, emb_out_ref, res_ref = take(emb_in), take(emb_out), take(residual)
    out_ref = take()
    stats_out = take(want_stats)
    out_a, out_b = take(talk), take(talk)
    wt_ref, xa, xb, scale_ref, offset_ref, sum_ref, sq_ref = (take() for _ in range(7))
    in_all, tx, out_all, edge, a_send, a_recv, b_send, b_recv, o_send, o_recv = (take(talk) for _ in range(10))
    if halo_in:
        halo_a, halo_b, i_send, i_recv = (take() for _ in range(4))
    step = pl.program_id(0)
    last_step = samples // 2 - 1
    me = lax.axis_index("sp")
    top, bottom = me == 0, me == peers - 1

    def normalize(dst, src, sample):
        scale = scale_ref[pl.ds(sample, 1), :]
        offset = offset_ref[pl.ds(sample, 1), :]

        def get_row(r, lo, hi):
            if r == 0:
                return halo_a[sample, :, lo:hi]
            if r == 17:
                return halo_b[sample, :, lo:hi]
            return src[0, r - 1, :, lo:hi]

        norm_rows(dst, get_row, scale, offset, range(18), top, bottom, 0, 17)

    def halo_group(i):
        first, size = HALO_GROUPS[i]
        part = pl.ds(first, size)
        return (
            RowSend(x_any.at[part, 15], halo_a.at[part], i_send.at[0, i], i_recv.at[0, i], me, peers, 1),
            RowSend(x_any.at[part, 0], halo_b.at[part], i_send.at[1, i], i_recv.at[1, i], me, peers, -1),
        )

    def edge_rows(pair):
        part = pl.ds(2 * pair, 2)
        return (
            RowSend(edge.at[part, 1], out_a.at[part], o_send.at[0, pair], o_recv.at[0, pair], me, peers, 1),
            RowSend(edge.at[part, 0], out_b.at[part], o_send.at[1, pair], o_recv.at[1, pair], me, peers, -1),
        )

    @pl.when(step == 0)
    def _():
        if talk:
            greet(me, peers)
            copies = to_all(stats_in, in_all, a_send, a_recv, me, peers)
            for copy in copies:
                copy.start()
            if halo_in:
                for i in range(len(HALO_GROUPS)):
                    for row in halo_group(i):
                        row.start()
            in_all[me] = stats_in[...]
        transpose_weights(w_ref, wt_ref)
        if talk:
            for copy in copies:
                copy.wait()
        bands = in_all if talk else stats_in
        total = bands[0]
        for d in range(1, peers):
            total = total + bands[d]
        total = total * (1.0 / count)
        var = pltpu.roll(total, LANE - GROUPS, 1) - total * total
        lane = lax.broadcasted_iota(jnp.int32, total.shape, 1)
        inv = jnp.where(lane < GROUPS, lax.rsqrt(var + EPS), 0.0)
        mean = jnp.where(lane < GROUPS, total, 0.0)
        expand = group_matrix(0, False)
        scale = f32_dot(inv, expand) * row_vector(gain_ref, layer)
        mean = f32_dot(mean, expand)
        if emb_in:
            mean = mean - emb_in_ref[0]
        offset = row_vector(shift_ref, layer) - mean * scale
        scale_ref[...] = scale * 0.5
        offset_ref[...] = offset * 0.5
        if halo_in:
            for row in halo_group(0):
                row.wait_recv()
        normalize(xa, x_first, 0)

    if halo_in:
        for i in range(1, len(HALO_GROUPS)):
            @pl.when(step == HALO_STEPS[i])
            def _():
                for row in halo_group(i):
                    row.wait_recv()
    if talk:
        @pl.when(step > 0)
        def _():
            for row in edge_rows(step - 1):
                row.start()

    bias = row_vector(bias_ref, layer)
    for sub, (cur, nxt, src) in enumerate(((xa, xb, x_odd), (xb, xa, x_even))):
        sample = step * 2 + sub
        nxt_sample = jnp.minimum(sample + 1, samples - 1)
        totals = []
        for half in range(2):
            total = None
            for dy in range(3):
                part = lax.dot_general(wt_ref[dy], cur[pl.ds((8 * half + dy) * COLS, 512), :], TRANS_B, preferred_element_type=F32)
                total = part if total is None else total + part
            totals.append(total)
        normalize(nxt, src, nxt_sample)
        tot = jnp.zeros((8, CH), F32)
        tot_sq = jnp.zeros((8, CH), F32)
        for pair in range(8):
            half, part = pair // 4, pair % 4
            u = (totals[half][:, part * LANE:(part + 1) * LANE].T + bias).astype(BF16)
            if residual:
                u = (res_ref[sub, 2 * pair:2 * pair + 2].reshape(LANE, CH).astype(F32) + u.astype(F32)).astype(BF16)
            out_ref[sub, 2 * pair:2 * pair + 2] = u.reshape(2, COLS, CH)
            if talk and pair == 0:
                edge[sample, 0] = u[:COLS]
            if talk and pair == 7:
                edge[sample, 1] = u[COLS:]
            if want_stats:
                v = u.astype(F32)
                if emb_out:
                    v = v + emb_out_ref[0, pl.ds(sample, 1), :]
                tot = tot + fold8(v)
                tot_sq = tot_sq + fold8(v * v)
        if want_stats:
            sum_ref[pl.ds(sample, 1), :] = tot.sum(axis=0, keepdims=True)
            sq_ref[pl.ds(sample, 1), :] = tot_sq.sum(axis=0, keepdims=True)

    if want_stats:
        @pl.when(step == last_step)
        def _():
            sums = group_sums(sum_ref, sq_ref)
            if not talk:
                stats_out[...] = sums
                return
            tx[...] = sums
            for row in edge_rows(last_step):
                row.start()
            out_all[me] = sums
            copies = to_all(tx, out_all, b_send, b_recv, me, peers)
            for copy in copies:
                copy.start()
            if halo_in:
                for i in range(len(HALO_GROUPS)):
                    for row in halo_group(i):
                        row.wait_send()
            for pair in range(samples // 2):
                for row in edge_rows(pair):
                    row.wait_send()
                    row.wait_recv()
            for copy in copies:
                copy.wait()
            stats_out[...] = out_all[...]


def group_sums(sum_ref, sq_ref):
    return f32_dot(sum_ref[...], group_matrix(0, True)) + f32_dot(sq_ref[...], group_matrix(GROUPS, True))


def once(shape):
    return pl.BlockSpec(shape, lambda g: (0,) * len(shape), pipeline_mode=pl.Buffered(1))


def layer_of(shape, layer):
    return pl.BlockSpec((1,) + shape[1:], lambda g: (layer,) + (0,) * (len(shape) - 1), pipeline_mode=pl.Buffered(1))


def conv_stage(x, halos, stats_in, gain, shift, bias, w, layer, peers, *, talk=None, emb_in=None, emb_out=None, residual=None, want_stats=True):
    samples, rows, cols, chans = x.shape
    count = float(rows * peers * cols * (chans // GROUPS))
    one = (1, rows, cols, chans)
    two = (2, rows, cols, chans)
    args = [x, x, x]
    specs = [
        once(one),
        pl.BlockSpec(one, lambda g: (2 * g + 1, 0, 0, 0)),
        pl.BlockSpec(one, lambda g: (jnp.minimum(2 * g + 2, samples - 1), 0, 0, 0)),
    ]
    halo_in = halos is None
    if halo_in:
        args.append(x)
        specs.append(pl.BlockSpec(memory_space=pl.ANY))
    else:
        args += list(halos)
        specs += [once(h.shape) for h in halos]
    args += [stats_in, gain, shift, bias, w]
    specs += [once(stats_in.shape), once(gain.shape), once(shift.shape), once(bias.shape), layer_of(w.shape, layer)]
    for emb in (emb_in, emb_out):
        if emb is not None:
            args.append(emb)
            specs.append(layer_of(emb.shape, layer))
    if residual is not None:
        args.append(residual)
        specs.append(pl.BlockSpec(two, lambda g: (g, 0, 0, 0)))
    out_shape = [jax.ShapeDtypeStruct(x.shape, BF16)]
    out_specs = [pl.BlockSpec(two, lambda g: (g, 0, 0, 0))]
    scratch = [
        pltpu.VMEM((3, CH, DEEP), BF16),
        pltpu.VMEM((18 * COLS, DEEP), BF16),
        pltpu.VMEM((18 * COLS, DEEP), BF16),
    ] + [pltpu.VMEM((samples, CH), F32)] * 4
    if want_stats:
        shape = (peers, samples, LANE) if talk is not None else (samples, LANE)
        out_shape.append(jax.ShapeDtypeStruct(shape, F32))
        out_specs.append(pl.BlockSpec(shape, lambda g: (0,) * len(shape)))
    if talk is not None:
        out_shape += [jax.ShapeDtypeStruct((samples, cols, chans), BF16)] * 2
        out_specs += [pl.BlockSpec(memory_space=pl.ANY)] * 2
        scratch += [
            pltpu.VMEM((peers, samples, LANE), F32),
            pltpu.VMEM((samples, LANE), F32),
            pltpu.VMEM((peers, samples, LANE), F32),
            pltpu.VMEM((samples, 2, cols, chans), BF16),
        ] + [pltpu.SemaphoreType.DMA((peers,))] * 4 + [pltpu.SemaphoreType.DMA((2, samples // 2))] * 2
    if halo_in:
        scratch += [pltpu.VMEM((samples, cols, chans), BF16)] * 2 + [pltpu.SemaphoreType.DMA((2, len(HALO_GROUPS)))] * 2
    body = functools.partial(stage_kernel, layer=layer, talk=talk is not None, halo_in=halo_in, emb_in=emb_in is not None, emb_out=emb_out is not None, residual=residual is not None, want_stats=want_stats, samples=samples, count=count, peers=peers)
    extra = {} if talk is None else {"collective_id": talk, "has_side_effects": True}
    return pl.pallas_call(
        body,
        grid=(samples // 2,),
        in_specs=specs,
        out_specs=out_specs,
        out_shape=out_shape,
        scratch_shapes=scratch,
        compiler_params=pltpu.CompilerParams(vmem_limit_bytes=VMEM_LIMIT, **extra),
        name="conv_stage_%d_%d" % (layer, 1 if talk is not None else 2),
    )(*args)


def first_kernel(lat_ref, halo_lat_a, halo_lat_b, w_ref, b_ref, time_ref, tw_ref, tb_ref, out_ref, halo_a, halo_b, stats_out, emb_ref, wt_ref, patch, sum_ref, sq_ref, *, peers, samples):
    step = pl.program_id(0)
    me = lax.axis_index("sp")

    @pl.when(step == 0)
    def _():
        parts = []
        for tap in range(9):
            parts.append(w_ref[tap // 3, tap % 3].astype(F32))
            parts.append(jnp.zeros((4, CH), F32))
        parts.append(jnp.zeros((LANE - 72, CH), F32))
        wt_ref[...] = jnp.concatenate(parts, axis=0).T.astype(BF16)[:, 0:80]
        time = time_ref[...].astype(F32)
        act = jax.nn.silu(time).astype(BF16)
        for i in range(2):
            emb = lax.dot_general(act, tw_ref[i], TRANS_B, preferred_element_type=F32)
            emb_ref[i] = emb + row_vector(tb_ref, i)

    lane = lax.broadcasted_iota(jnp.int32, (4, LANE), 1)
    col = lane & 63
    bias = b_ref[...].astype(F32).reshape(1, CH)
    zero4 = jnp.zeros((4, LANE), F32)
    for sub in range(2):
        sample = 2 * step + sub
        shifted = {}
        for r in range(20):
            if r < 2:
                row = halo_lat_a[sample, r].astype(F32)
                row = jnp.where(me == 0, jnp.zeros_like(row), row)
            elif r > 17:
                row = halo_lat_b[sample, r - 18].astype(F32)
                row = jnp.where(me == peers - 1, jnp.zeros_like(row), row)
            else:
                row = lat_ref[sub, r - 2].astype(F32)
            both = jnp.concatenate([row, row], axis=-1)
            shifted[r, 0] = jnp.where(col == 0, 0.0, pltpu.roll(both, 1, 1))
            shifted[r, 1] = both
            shifted[r, 2] = jnp.where(col == 63, 0.0, pltpu.roll(both, 127, 1))
        for pair in range(9):
            parts = []
            for dy in range(3):
                for dx in range(3):
                    parts.append(jnp.where(lane < COLS, shifted[2 * pair + dy, dx], shifted[2 * pair + 1 + dy, dx]))
                    parts.append(zero4)
            parts += [zero4] * 2
            patch[sub, :, pair * LANE:(pair + 1) * LANE] = jnp.concatenate(parts, axis=0).astype(BF16)
        tot = jnp.zeros((8, CH), F32)
        tot_sq = jnp.zeros((8, CH), F32)
        for pair in range(9):
            if pair % 3 == 0:
                total = jnp.dot(wt_ref[...], patch[sub, :, pair * LANE:(pair + 3) * LANE], preferred_element_type=F32)
            lo = (pair % 3) * LANE
            u = (total[:, lo:lo + LANE].T + bias).astype(BF16)
            upper, lower = u[:COLS], u[COLS:]
            if pair == 0:
                halo_a[sub] = upper
            else:
                out_ref[sub, 2 * pair - 1] = upper
            if pair == 8:
                halo_b[sub] = lower
            else:
                out_ref[sub, 2 * pair] = lower
            v = u.astype(F32)
            if pair == 0:
                v = v[COLS:]
            if pair == 8:
                v = v[:COLS]
            tot = tot + fold8(v)
            tot_sq = tot_sq + fold8(v * v)
        sum_ref[pl.ds(sample, 1), :] = tot.sum(axis=0, keepdims=True)
        sq_ref[pl.ds(sample, 1), :] = tot_sq.sum(axis=0, keepdims=True)

    @pl.when(step == samples // 2 - 1)
    def _():
        stats_out[...] = group_sums(sum_ref, sq_ref)


def first_conv(lat, halos, w_in, b_in, time_emb, temb_w, temb_b, peers):
    samples = lat.shape[0]
    return pl.pallas_call(
        functools.partial(first_kernel, peers=peers, samples=samples),
        grid=(samples // 2,),
        in_specs=[pl.BlockSpec((2,) + lat.shape[1:], lambda s: (s, 0, 0, 0))] + [once(a.shape) for a in (halos[0], halos[1], w_in, b_in, time_emb, temb_w, temb_b)],
        out_specs=[
            pl.BlockSpec((2, ROWS, COLS, CH), lambda s: (s, 0, 0, 0)),
            pl.BlockSpec((2, COLS, CH), lambda s: (s, 0, 0)),
            pl.BlockSpec((2, COLS, CH), lambda s: (s, 0, 0)),
            pl.BlockSpec((samples, LANE), lambda s: (0, 0)),
            pl.BlockSpec((2, samples, CH), lambda s: (0, 0, 0)),
        ],
        out_shape=[
            jax.ShapeDtypeStruct((samples, ROWS, COLS, CH), BF16),
            jax.ShapeDtypeStruct((samples, COLS, CH), BF16),
            jax.ShapeDtypeStruct((samples, COLS, CH), BF16),
            jax.ShapeDtypeStruct((samples, LANE), F32),
            jax.ShapeDtypeStruct((2, samples, CH), F32),
        ],
        scratch_shapes=[
            pltpu.VMEM((CH, 80), BF16),
            pltpu.VMEM((2, 80, 18 * COLS), BF16),
            pltpu.VMEM((samples, CH), F32),
            pltpu.VMEM((samples, CH), F32),
        ],
        compiler_params=pltpu.CompilerParams(vmem_limit_bytes=VMEM_LIMIT),
        name="conv_in",
    )(lat, halos[0], halos[1], w_in, b_in, time_emb, temb_w, temb_b)


DOWN_GROUPS = ((0, 2), (2, 2), (4, 4), (8, 8))
DOWN_STEPS = (None, 1, 2, 4)


def down_kernel(x_ref, x_any, bias_ref, w_ref, out_ref, wt_ref, xe, xo, wide, halo, send, recv, *, peers, samples):
    step = pl.program_id(0)
    me = lax.axis_index("sp")

    def group(i):
        first, size = DOWN_GROUPS[i]
        part = pl.ds(first, size)
        return RowSend(x_any.at[part, 15], halo.at[part], send.at[i], recv.at[i], me, peers, 1)

    @pl.when(step == 0)
    def _():
        greet(me, peers)
        for i in range(len(DOWN_GROUPS)):
            group(i).start()
        transpose_weights(w_ref, wt_ref)
        group(0).wait_recv()

    for i in range(1, len(DOWN_GROUPS)):
        @pl.when(step == DOWN_STEPS[i])
        def _():
            group(i).wait_recv()

    bias = bias_ref[...].astype(F32).reshape(1, CH)
    for sub in range(2):
        for r in range(17):
            dst, row0 = (xe, 32 * (r // 2)) if r % 2 == 0 else (xo, 32 * (r // 2))
            for tile, (lo, hi) in enumerate(WIDE):
                v = halo[step * 2 + sub, :, lo:hi] if r == 0 else x_ref[sub, r - 1, :, lo:hi]
                v = v.astype(F32)
                if r == 0:
                    v = jnp.where(me == 0, jnp.zeros_like(v), v)
                slot = (r * 2 + tile) % 8
                parts = []
                for piece in range((hi - lo + 127) // LANE):
                    first, end = piece * LANE, min(hi - lo, piece * LANE + LANE)
                    wide[slot, piece, :, 0:end - first] = v[:, first:end]
                    parts.append([wide[slot, piece, pl.ds(odd, 32, stride=2), 0:end - first] for odd in range(2)])
                even = jnp.concatenate([p[0] for p in parts], axis=-1)
                odd = jnp.concatenate([p[1] for p in parts], axis=-1)
                padded = jnp.concatenate([odd, jnp.zeros((8, hi - lo), F32)], axis=0)
                put_shifted(dst.at[sub], row0, 32, tile, pltpu.roll(padded, 1, 0)[:32], even, odd)
        total = None
        for dy, src in enumerate((xe.at[sub, pl.ds(0, FULL)], xo.at[sub], xe.at[sub, pl.ds(32, FULL)])):
            part = lax.dot_general(wt_ref[dy], src[...], TRANS_B, preferred_element_type=F32)
            total = part if total is None else total + part
        for part in range(2):
            u = (total[:, part * LANE:(part + 1) * LANE].T + bias).astype(BF16)
            out_ref[sub, 4 * part:4 * part + 4] = u.reshape(4, 32, CH)

    @pl.when(step == samples // 2 - 1)
    def _():
        for i in range(len(DOWN_GROUPS)):
            group(i).wait_send()


def down_conv(x, w, bias, peers, collective_id):
    samples = x.shape[0]
    return pl.pallas_call(
        functools.partial(down_kernel, peers=peers, samples=samples),
        grid=(samples // 2,),
        in_specs=[pl.BlockSpec((2, ROWS, COLS, CH), lambda g: (g, 0, 0, 0)), pl.BlockSpec(memory_space=pl.ANY), once(bias.shape), once(w.shape)],
        out_specs=pl.BlockSpec((2, 8, 32, CH), lambda g: (g, 0, 0, 0)),
        out_shape=jax.ShapeDtypeStruct((samples, 8, 32, CH), BF16),
        scratch_shapes=[
            pltpu.VMEM((3, CH, DEEP), BF16),
            pltpu.VMEM((2, 9 * 32, DEEP), BF16),
            pltpu.VMEM((2, 8 * 32, DEEP), BF16),
            pltpu.VMEM((8, 2, COLS, LANE), F32),
            pltpu.VMEM((samples, COLS, CH), BF16),
            pltpu.SemaphoreType.DMA((len(DOWN_GROUPS),)),
            pltpu.SemaphoreType.DMA((len(DOWN_GROUPS),)),
        ],
        compiler_params=pltpu.CompilerParams(vmem_limit_bytes=VMEM_LIMIT, collective_id=collective_id, has_side_effects=True),
        name="down",
    )(x, x, bias, w)


def latent_kernel(lat_ref, halo_a, halo_b, send, recv, *, peers):
    me = lax.axis_index("sp")
    greet(me, peers)
    last = lat_ref.shape[1] - 2
    rows = (
        RowSend(lat_ref.at[:, pl.ds(last, 2)], halo_a, send.at[0], recv.at[0], me, peers, 1),
        RowSend(lat_ref.at[:, pl.ds(0, 2)], halo_b, send.at[1], recv.at[1], me, peers, -1),
    )
    for row in rows:
        row.start()
    for row in rows:
        row.wait_send()
        row.wait_recv()


def latent_halos(lat, peers, collective_id):
    shape = jax.ShapeDtypeStruct((lat.shape[0], 2) + lat.shape[2:], lat.dtype)
    return pl.pallas_call(
        functools.partial(latent_kernel, peers=peers),
        in_specs=[pl.BlockSpec(memory_space=pl.ANY)],
        out_specs=[pl.BlockSpec(memory_space=pl.ANY)] * 2,
        out_shape=[shape, shape],
        scratch_shapes=[pltpu.SemaphoreType.DMA((2,)), pltpu.SemaphoreType.DMA((2,))],
        compiler_params=pltpu.CompilerParams(collective_id=collective_id, has_side_effects=True),
        name="latent_halos",
    )(lat)


def solution(mesh):
    peers = mesh.shape["sp"]

    def band_program(latent, time_emb, w_in, b_in, gn1_scale, gn1_shift, conv1_w, conv1_b, temb_w, temb_b, gn2_scale, gn2_shift, conv2_w, conv2_b, down_w, down_b):
        lat = latent.transpose(0, 1, 3, 2)
        hidden, halo_a, halo_b, stats, embs = first_conv(lat, latent_halos(lat, peers, 0), w_in, b_in, time_emb, temb_w.transpose(0, 2, 1), temb_b, peers)
        outputs = [hidden]
        for i in range(2):
            halos = (halo_a, halo_b) if i == 0 else None
            branch, stats_all, halo_a, halo_b = conv_stage(hidden, halos, stats, gn1_scale, gn1_shift, conv1_b, conv1_w, i, peers, talk=i + 1, emb_out=embs)
            got = conv_stage(branch, (halo_a, halo_b), stats_all, gn2_scale, gn2_shift, conv2_b, conv2_w, i, peers, emb_in=embs, residual=hidden, want_stats=i == 0)
            hidden = got[0]
            stats = got[1] if i == 0 else None
            outputs.append(hidden)
        outputs.append(down_conv(hidden, down_w[None], down_b, peers, 3))
        return tuple(outputs)

    band = P("dp", "sp", None, None)
    return jax.shard_map(band_program, mesh=mesh, in_specs=(band, P("dp", None)) + (P(),) * 14, out_specs=(band,) * 4, check_vma=False)
```
